8 devices in a mesh: dp: 2 (over z, y), pp: 4 (over x, core).
Axes of the slice: x: 2, y: 2, z: 1, core: 2. Of those that a mesh axis runs over, the one named last changes fastest.
Arguments:
- x_in: bfloat16 [6, 8, 128, 2432], P('dp'), parts along dimension 0
- cond_vec: bfloat16 [6, 2432], P('dp'), parts along dimension 0
- pos_ids: int32 [8, 128, 3], replicated
- w_mod: bfloat16 [4, 2432, 7296], P('pp')
- b_mod: bfloat16 [4, 7296], P('pp')
- w_one: bfloat16 [4, 2432, 17024], P('pp')
- b_one: bfloat16 [4, 17024], P('pp')
- qk_scale: bfloat16 [4, 2, 64], P('pp')
- w_two: bfloat16 [4, 12160, 2432], P('pp')
- b_two: bfloat16 [4, 2432], P('pp')
- k_prev: bfloat16 [4, 6, 8, 128, 2432], P('pp', 'dp'), parts along dimension 1
- v_prev: bfloat16 [4, 6, 8, 128, 2432], P('pp', 'dp'), parts along dimension 1
Outputs:
- output 1: bfloat16 [6, 8, 128, 2432], P('dp', 'pp'), parts along dimension 0
- output 2: bfloat16 [4, 6, 8, 128, 2432], P('pp', 'dp'), parts along dimension 1
- output 3: bfloat16 [4, 6, 8, 128, 2432], P('pp', 'dp'), parts along dimension 1
There are 2 independent parts. The reference program is written for one: setup_inputs(seed, part) draws one part's arguments, and reference() takes and returns one part's arrays. A program takes and returns all parts, laid end to end along the dimension named above; an argument that names none is the same for every part.
All inputs are finite; a program needn't handle non-finite values.
Results may differ from the reference program's by a relative error of at most 0.0108307.
Values are sent between devices in bfloat16 or wider.
A program may use at most 1 GiB of HBM per device.

```python
import math
import jax
import jax.numpy as jnp
from jax import lax

WIDTH = 2432
HEAD_DIM = 64
MLP_DIM = 9728
BATCH = 3
PATCHES = 8
PATCH_TOK = 128
LAYERS = 4
GRID_W = 64

SEQ = PATCHES * PATCH_TOK
QK_GAIN = math.log(SEQ / 16) ** 0.25


def make_ids(key):
    id_keys = jax.random.split(key, 3)
    frame_idx = jax.random.randint(id_keys[0], (), 0, 8, dtype=jnp.int32)
    row_off = jax.random.randint(id_keys[1], (), 0, 64, dtype=jnp.int32)
    col_off = jax.random.randint(id_keys[2], (), 0, 64, dtype=jnp.int32)
    img_index = jnp.arange(SEQ - PATCH_TOK, dtype=jnp.int32)
    img_ids = jnp.stack([jnp.zeros_like(img_index) + frame_idx, row_off + img_index // GRID_W, col_off + img_index % GRID_W], axis=-1)
    txt_ids = jnp.zeros((PATCH_TOK, 3), jnp.int32)
    return jnp.concatenate([txt_ids, img_ids], axis=0).reshape(PATCHES, PATCH_TOK, 3)


def setup_inputs(seed: int = 0, part: int = 0) -> dict:
    shared = jax.random.split(jax.random.key(seed), 8)
    own_keys = jax.random.split(jax.random.fold_in(jax.random.key(seed + 1), part), 4)
    proj_dim = 3 * WIDTH + MLP_DIM
    act_shape = (BATCH, PATCHES, PATCH_TOK, WIDTH)
    buf_shape = (LAYERS, BATCH, PATCHES, PATCH_TOK, WIDTH)
    row_gain = jnp.where(jnp.arange(WIDTH + MLP_DIM) < WIDTH, 2.0, 1.0)[None, :, None]
    return {
        'x_in': jax.random.normal(own_keys[0], act_shape, jnp.float32).astype(jnp.bfloat16),
        'cond_vec': jax.random.normal(own_keys[1], (BATCH, WIDTH), jnp.float32).astype(jnp.bfloat16),
        'pos_ids': make_ids(shared[0]),
        'w_mod': (jax.random.normal(shared[1], (LAYERS, WIDTH, 3 * WIDTH), jnp.float32) * WIDTH ** -0.5).astype(jnp.bfloat16),
        'b_mod': (0.5 * jax.random.normal(shared[2], (LAYERS, 3 * WIDTH), jnp.float32)).astype(jnp.bfloat16),
        'w_one': (jax.random.normal(shared[3], (LAYERS, WIDTH, proj_dim), jnp.float32) * WIDTH ** -0.5).astype(jnp.bfloat16),
        'b_one': (0.5 * jax.random.normal(shared[4], (LAYERS, proj_dim), jnp.float32)).astype(jnp.bfloat16),
        'qk_scale': (QK_GAIN * (1.0 + 0.3 * jax.random.normal(shared[5], (LAYERS, 2, HEAD_DIM), jnp.float32))).astype(jnp.bfloat16),
        'w_two': (jax.random.normal(shared[6], (LAYERS, WIDTH + MLP_DIM, WIDTH), jnp.float32) * (WIDTH + MLP_DIM) ** -0.5 * row_gain).astype(jnp.bfloat16),
        'b_two': (0.5 * jax.random.normal(shared[7], (LAYERS, WIDTH), jnp.float32)).astype(jnp.bfloat16),
        'k_prev': (QK_GAIN * jax.random.normal(own_keys[2], buf_shape, jnp.float32)).astype(jnp.bfloat16),
        'v_prev': jax.random.normal(own_keys[3], buf_shape, jnp.float32).astype(jnp.bfloat16),
    }


def layer_norm(hidden):
    act32 = hidden.astype(jnp.float32)
    centered = act32 - jnp.mean(act32, axis=-1, keepdims=True)
    return centered * lax.rsqrt(jnp.mean(centered * centered, axis=-1, keepdims=True) + 1e-6)


def rope_tables(pos_ids, head_dim):
    axis_zero = head_dim // 8
    axis_rest = (head_dim - axis_zero) // 2
    pieces = []
    for axis_idx, axis_dim in enumerate((axis_zero, axis_rest, head_dim - axis_zero - axis_rest)):
        axis_freqs = 1.0 / (10000.0 ** (jnp.arange(0, axis_dim, 2, dtype=jnp.float32) / axis_dim))
        pieces.append(pos_ids[..., axis_idx:axis_idx + 1].astype(jnp.float32) * axis_freqs)
    angles = jnp.concatenate(pieces, axis=-1)[..., None, :]
    return jnp.cos(angles), jnp.sin(angles)


def rms_rope(raw_heads, norm_gain, cos_tab, sin_tab):
    raw32 = raw_heads.astype(jnp.float32)
    normed = raw32 * lax.rsqrt(jnp.mean(raw32 * raw32, axis=-1, keepdims=True) + 1e-6) * norm_gain.astype(jnp.float32)
    pair_view = normed.reshape(normed.shape[:-1] + (normed.shape[-1] // 2, 2))
    even_part = pair_view[..., 0]
    odd_part = pair_view[..., 1]
    rotated = jnp.stack([cos_tab * even_part - sin_tab * odd_part, sin_tab * even_part + cos_tab * odd_part], axis=-1)
    return rotated.reshape(raw_heads.shape).astype(jnp.bfloat16)


def reference(x_in, cond_vec, pos_ids, w_mod, b_mod, w_one, b_one, qk_scale, w_two, b_two, k_prev, v_prev):
    batch_size, patches, patch_tok, width = x_in.shape
    head_dim = qk_scale.shape[-1]
    head_count = width // head_dim
    seq_len = patches * patch_tok
    score_scale = 1.0 / math.sqrt(head_dim)
    head_shape = (batch_size, patches, patch_tok, head_count, head_dim)
    cos_tab, sin_tab = rope_tables(pos_ids, head_dim)
    cond_act = jax.nn.silu(cond_vec.astype(jnp.float32)).astype(jnp.bfloat16)
    patch_rank = jnp.arange(patches)

    def layer_step(hidden, layer_in):
        mod_w, mod_b, one_w, one_b, norm_gain, two_w, two_b, k_old, v_old = layer_in
        mod_vals = (jnp.dot(cond_act, mod_w, preferred_element_type=jnp.float32) + mod_b.astype(jnp.float32))[:, None, None, :]
        shift_mod = mod_vals[..., :width]
        scale_mod = mod_vals[..., width:2 * width]
        gate_mod = mod_vals[..., 2 * width:]
        h_mod = (layer_norm(hidden) * (1.0 + scale_mod) + shift_mod).astype(jnp.bfloat16)
        proj_out = (jnp.dot(h_mod.reshape(-1, width), one_w, preferred_element_type=jnp.float32) + one_b.astype(jnp.float32)).astype(jnp.bfloat16)
        proj_out = proj_out.reshape(batch_size, patches, patch_tok, -1)
        q_rot = rms_rope(proj_out[..., :width].reshape(head_shape), norm_gain[0], cos_tab, sin_tab)
        k_rot = rms_rope(proj_out[..., width:2 * width].reshape(head_shape), norm_gain[1], cos_tab, sin_tab)
        v_new = proj_out[..., 2 * width:3 * width].reshape(head_shape)
        k_prior = k_old.reshape(head_shape)
        v_prior = v_old.reshape(head_shape)

        def attend(patch_idx):
            is_fresh = (patch_rank <= patch_idx)[None, :, None, None, None]
            key_all = jnp.where(is_fresh, k_rot, k_prior).reshape(batch_size, seq_len, head_count, head_dim).astype(jnp.float32)
            val_all = jnp.where(is_fresh, v_new, v_prior).reshape(batch_size, seq_len, head_count, head_dim).astype(jnp.float32)
            q_patch = lax.dynamic_index_in_dim(q_rot, patch_idx, axis=1, keepdims=False).astype(jnp.float32)
            scores = jnp.einsum('bqhd,bkhd->bhqk', q_patch, key_all) * score_scale
            prob_bf = jax.nn.softmax(scores, axis=-1).astype(jnp.bfloat16)
            return jnp.einsum('bhqk,bkhd->bqhd', prob_bf.astype(jnp.float32), val_all).astype(jnp.bfloat16)

        attn_out = jnp.moveaxis(lax.map(attend, patch_rank), 0, 1).reshape(x_in.shape)
        mlp_act = jax.nn.gelu(proj_out[..., 3 * width:].astype(jnp.float32), approximate=True).astype(jnp.bfloat16)
        joined = jnp.concatenate([attn_out, mlp_act], axis=-1).reshape(-1, two_w.shape[0])
        block_out = jnp.dot(joined, two_w, preferred_element_type=jnp.float32).reshape(x_in.shape) + two_b.astype(jnp.float32)
        hidden_new = (hidden.astype(jnp.float32) + gate_mod * block_out).astype(jnp.bfloat16)
        return hidden_new, (k_rot.reshape(x_in.shape), v_new.reshape(x_in.shape))

    x_out, (k_new, v_new) = lax.scan(layer_step, x_in, (w_mod, b_mod, w_one, b_one, qk_scale, w_two, b_two, k_prev, v_prev))
    return x_out, k_new, v_new
```

```python
import functools
import math
import jax
import jax.numpy as jnp
from jax import lax
from jax.experimental import pallas as pl
from jax.experimental.pallas import tpu as pltpu
from jax.sharding import PartitionSpec as P

UNITS = 2
WEIGHT_SLOTS = 2
COL_BLOCK = 2432
LANES = 128


def rope_tables(pos_ids, head_dim):
    axis_zero = head_dim // 8
    axis_rest = (head_dim - axis_zero) // 2
    pieces = []
    for axis_idx, axis_dim in enumerate((axis_zero, axis_rest, head_dim - axis_zero - axis_rest)):
        axis_freqs = 1.0 / (10000.0 ** (jnp.arange(0, axis_dim, 2, dtype=jnp.float32) / axis_dim))
        pieces.append(pos_ids[..., axis_idx:axis_idx + 1].astype(jnp.float32) * axis_freqs)
    angles = jnp.concatenate(pieces, axis=-1)
    return jnp.cos(angles), jnp.sin(angles)


def col_blocks(width, body):
    full = width // COL_BLOCK

    def step(blk, carry):
        body(pl.multiple_of(blk * COL_BLOCK, LANES), COL_BLOCK)
        return carry

    lax.fori_loop(0, full, step, 0)
    if width % COL_BLOCK:
        body(full * COL_BLOCK, width % COL_BLOCK)


def stage_kernel(stages, units, head_dim,
                 x_in, mod, b_one, gains, cos_tab, sin_tab, ones_bd, b_two, w_one, w_two, k_prev, v_prev,
                 x_out, k_new, v_new, recv_x,
                 w_buf, k_buf, v_buf, x_buf, qkv, joined, acc, o_buf,
                 w_sem, kv_sem, x_sem, kv_out_sem, send_sem, local_sem, recv_sem, out_sem):
    stage = lax.axis_index('pp')
    samples, seq, width = x_in.shape
    rows = x_buf.shape[0]
    patch_tok = rows // units
    parts = seq // rows
    chunks = samples * parts
    slots = w_buf.shape[0]
    tiles_one = w_one.shape[1] // width
    tiles_two = w_two.shape[0] // width
    tiles = tiles_one + tiles_two
    last = stages - 1

    barrier = pltpu.get_barrier_semaphore()
    for hop in range(1, stages):
        pl.semaphore_signal(barrier, inc=1, device_id={'pp': lax.rem(stage + hop, stages)}, device_id_type=pl.DeviceIdType.MESH)
    pl.semaphore_wait(barrier, stages - 1)

    def tile_start(g):
        t = lax.rem(g, tiles)
        slot = lax.rem(g, slots)

        @pl.when(t < tiles_one)
        def _():
            pltpu.make_async_copy(w_one.at[:, pl.ds(pl.multiple_of(t * width, LANES), width)], w_buf.at[slot], w_sem.at[slot]).start()

        @pl.when(t >= tiles_one)
        def _():
            pltpu.make_async_copy(w_two.at[pl.ds(pl.multiple_of((t - tiles_one) * width, LANES), width), :], w_buf.at[slot], w_sem.at[slot]).start()

    def tile_wait(g):
        slot = lax.rem(g, slots)
        pltpu.make_async_copy(w_two.at[pl.ds(0, width), :], w_buf.at[slot], w_sem.at[slot]).wait()
        return slot

    def tile_done(g):
        @pl.when(g + slots < chunks * tiles)
        def _():
            tile_start(g + slots)

    for g0 in range(slots):
        tile_start(g0)

    def send_copy(c):
        s, part = lax.div(c, parts), lax.rem(c, parts)
        return pltpu.make_async_remote_copy(
            src_ref=o_buf, dst_ref=recv_x.at[s, pl.ds(pl.multiple_of(part * rows, LANES), rows), :],
            send_sem=send_sem, recv_sem=recv_sem.at[c],
            device_id={'pp': lax.rem(stage + 1, stages)}, device_id_type=pl.DeviceIdType.MESH)

    def out_copy(c):
        s, part = lax.div(c, parts), lax.rem(c, parts)
        return pltpu.make_async_remote_copy(
            src_ref=o_buf, dst_ref=x_out.at[s], send_sem=send_sem, recv_sem=out_sem.at[s],
            device_id={'pp': part}, device_id_type=pl.DeviceIdType.MESH)

    def local_copy(c):
        return pltpu.make_async_copy(o_buf, x_out.at[lax.div(c, parts)], local_sem)

    def out_start(c):
        part = lax.rem(c, parts)

        @pl.when(stage < last)
        def _():
            send_copy(c).start()

        @pl.when((stage == last) & (part < last))
        def _():
            out_copy(c).start()

        @pl.when((stage == last) & (part == last))
        def _():
            local_copy(c).start()

    def out_wait(c):
        part = lax.rem(c, parts)

        @pl.when(stage < last)
        def _():
            send_copy(c).wait_send()

        @pl.when((stage == last) & (part < last))
        def _():
            out_copy(c).wait_send()

        @pl.when((stage == last) & (part == last))
        def _():
            local_copy(c).wait()

    lane = lax.broadcasted_iota(jnp.int32, (patch_tok, LANES), 1)
    low_half = (lane < head_dim)
    low_bf = low_half.astype(jnp.float32).astype(jnp.bfloat16)
    high_bf = (1.0 - low_half.astype(jnp.float32)).astype(jnp.bfloat16)

    def chunk_body(c, carry):
        s, part = lax.div(c, parts), lax.rem(c, parts)
        row0 = pl.multiple_of(part * rows, LANES)
        base = c * tiles
        span = pl.ds(row0, rows)

        def prev_copies():
            return (pltpu.make_async_copy(k_prev.at[s], k_buf, kv_sem.at[0]),
                    pltpu.make_async_copy(v_prev.at[s], v_buf, kv_sem.at[1]))

        @pl.when(part == 0)
        def _():
            for cp in prev_copies():
                cp.start()

        @pl.when(stage == 0)
        def _():
            cp = pltpu.make_async_copy(x_in.at[s, span, :], x_buf, x_sem)
            cp.start()
            cp.wait()

        @pl.when(stage > 0)
        def _():
            send_copy(c).wait_recv()
            cp = pltpu.make_async_copy(recv_x.at[s, span, :], x_buf, x_sem)
            cp.start()
            cp.wait()

        norm_rows = 16

        def norm_step(r, carry):
            at = pl.ds(pl.multiple_of(r * norm_rows, norm_rows), norm_rows)
            act = x_buf[at, :].astype(jnp.float32)
            centered = act - jnp.mean(act, axis=-1, keepdims=True)
            normed = centered * lax.rsqrt(jnp.mean(centered * centered, axis=-1, keepdims=True) + 1e-6)
            joined[0, at, :] = (normed * (1.0 + mod[s, 1:2, :]) + mod[s, 0:1, :]).astype(jnp.bfloat16)
            return carry

        lax.fori_loop(0, rows // norm_rows, norm_step, 0, unroll=2)

        def proj(slot, j, off, size):
            cols = pl.ds(off, size)
            out = jnp.dot(joined[0], w_buf[slot, :, cols], preferred_element_type=jnp.float32)
            return (out + b_one[j, :, cols]).astype(jnp.bfloat16)

        def head_tile(j, carry):
            slot = tile_wait(base + j)
            even = (lax.broadcasted_iota(jnp.int32, (rows, LANES), 1) & 1) == 0

            def body(off, size):
                raw = proj(slot, j, off, size).astype(jnp.float32)
                cos_v = cos_tab[span, :]
                sin_v = sin_tab[span, :]
                for lo in range(0, size, 2 * LANES):
                    wide = min(2 * LANES, size - lo)
                    sub = raw[:, lo:lo + wide]
                    sq = sub * sub
                    ones = ones_bd[:wide, :wide]
                    sq0 = sq.astype(jnp.bfloat16)
                    rem1 = sq - sq0.astype(jnp.float32)
                    sq1 = rem1.astype(jnp.bfloat16)
                    sq2 = (rem1 - sq1.astype(jnp.float32)).astype(jnp.bfloat16)
                    total = jnp.dot(sq0, ones, preferred_element_type=jnp.float32)
                    total += jnp.dot(sq1, ones, preferred_element_type=jnp.float32)
                    total += jnp.dot(sq2, ones, preferred_element_type=jnp.float32)
                    inv = lax.rsqrt(total * (1.0 / head_dim) + 1e-6)
                    for l2 in range(0, wide, LANES):
                        one = sub[:, l2:l2 + LANES] * inv[:, l2:l2 + LANES] * gains[j]
                        swapped = jnp.where(even, pltpu.roll(one, LANES - 1, 1), pltpu.roll(one, 1, 1))
                        rot = one * cos_v + swapped * sin_v
                        qkv[j, :, pl.ds(off + lo + l2, LANES)] = rot.astype(jnp.bfloat16)

            col_blocks(width, body)
            tile_done(base + j)
            return carry

        lax.fori_loop(0, 2, head_tile, 0)

        slot_v = tile_wait(base + 2)

        def value_body(off, size):
            qkv[2, :, pl.ds(off, size)] = proj(slot_v, 2, off, size)

        col_blocks(width, value_body)
        tile_done(base + 2)

        def fresh_copies():
            return (pltpu.make_async_copy(qkv.at[1], k_new.at[s, span, :], kv_out_sem.at[0]),
                    pltpu.make_async_copy(qkv.at[2], v_new.at[s, span, :], kv_out_sem.at[1]))

        for cp in fresh_copies():
            cp.start()

        def mlp_tile(j, carry):
            slot = tile_wait(base + j)

            def body(off, size):
                pre = proj(slot, j, off, size).astype(jnp.float32)
                joined[j - 2, :, pl.ds(off, size)] = jax.nn.gelu(pre, approximate=True).astype(jnp.bfloat16)

            col_blocks(width, body)
            tile_done(base + j)
            return carry

        lax.fori_loop(3, tiles_one, mlp_tile, 0)

        @pl.when(part == 0)
        def _():
            for cp in prev_copies():
                cp.wait()

        def unit_step(u, carry):
            q_rows = pl.ds(pl.multiple_of(u * patch_tok, LANES), patch_tok)
            key_rows = pl.ds(pl.multiple_of(row0 + u * patch_tok, LANES), patch_tok)
            k_buf[key_rows, :] = qkv[1, q_rows, :]
            v_buf[key_rows, :] = qkv[2, q_rows, :]

            def pair(off):
                cols = pl.ds(off, LANES)
                q2 = qkv[0, q_rows, cols]
                both = jnp.concatenate([q2 * low_bf, q2 * high_bf], axis=0)
                scores = lax.dot_general(both, k_buf[:, cols], (((1,), (1,)), ((), ())), preferred_element_type=jnp.float32)
                top = jnp.max(scores, axis=-1, keepdims=True)
                ex = jnp.exp(scores - top)
                prob = (ex * (1.0 / jnp.sum(ex, axis=-1, keepdims=True))).astype(jnp.bfloat16)
                mixed = jnp.dot(prob, v_buf[:, cols], preferred_element_type=jnp.float32)
                joined[0, q_rows, cols] = jnp.where(low_half, mixed[:patch_tok], mixed[patch_tok:]).astype(jnp.bfloat16)

            pairs = width // LANES
            group = 3

            def pair_step(i, carry):
                for k in range(group):
                    pair(pl.multiple_of((i * group + k) * LANES, LANES))
                return carry

            lax.fori_loop(0, pairs // group, pair_step, 0)
            for k in range(pairs - pairs % group, pairs):
                pair(k * LANES)
            return carry

        lax.fori_loop(0, units, unit_step, 0)

        def two_tile(j, carry):
            slot = tile_wait(base + tiles_one + j)

            def body(off, size):
                cols = pl.ds(off, size)
                part_sum = jnp.dot(joined[j], w_buf[slot, :, cols], preferred_element_type=jnp.float32)
                acc[:, cols] = acc[:, cols] + part_sum

            col_blocks(width, body)
            tile_done(base + tiles_one + j)
            return carry

        acc[...] = jnp.zeros_like(acc)
        lax.fori_loop(0, tiles_two, two_tile, 0)

        for cp in fresh_copies():
            cp.wait()

        @pl.when(c > 0)
        def _():
            out_wait(c - 1)

        def res_step(r, carry):
            at = pl.ds(pl.multiple_of(r * norm_rows, norm_rows), norm_rows)
            block_out = acc[at, :] + b_two[...]
            o_buf[at, :] = (x_buf[at, :].astype(jnp.float32) + mod[s, 2:3, :] * block_out).astype(jnp.bfloat16)
            return carry

        lax.fori_loop(0, rows // norm_rows, res_step, 0, unroll=2)
        out_start(c)
        return carry

    lax.fori_loop(0, chunks, chunk_body, 0)
    out_wait(chunks - 1)

    @pl.when(stage < last)
    def _():
        for s in range(samples):
            out_copy(s * parts).wait_recv()


def solution(mesh):
    stages = mesh.shape['pp']

    def stage_program(x_in, cond_vec, pos_ids, w_mod, b_mod, w_one, b_one, qk_scale, w_two, b_two, k_prev, v_prev):
        samples, patches, patch_tok, width = x_in.shape
        head_dim = qk_scale.shape[-1]
        seq = patches * patch_tok
        rows = UNITS * patch_tok
        chunks = samples * seq // rows
        tiles_one = w_one.shape[2] // width
        tiles_two = w_two.shape[1] // width
        cond_act = jax.nn.silu(cond_vec.astype(jnp.float32)).astype(jnp.bfloat16)
        mod = jnp.dot(cond_act, w_mod[0], preferred_element_type=jnp.float32) + b_mod.astype(jnp.float32)
        mod = mod.reshape(samples, 3, width)
        cos_tab, sin_tab = rope_tables(pos_ids.reshape(seq, 3), head_dim)
        heads_in_lane = LANES // head_dim
        cos_tab = jnp.tile(jnp.repeat(cos_tab, 2, axis=-1), (1, heads_in_lane))
        sin_tab = jnp.stack([-sin_tab, sin_tab], axis=-1).reshape(seq, head_dim)
        sin_tab = jnp.tile(sin_tab, (1, heads_in_lane))
        scale = jnp.array([1.0 / math.sqrt(head_dim), 1.0], jnp.float32)
        gains = jnp.tile(qk_scale[0].astype(jnp.float32) * scale[:, None], (1, heads_in_lane)).reshape(2, 1, LANES)
        group = jnp.arange(2 * LANES) // head_dim
        ones_bd = (group[:, None] == group[None, :]).astype(jnp.bfloat16)
        vmem = pl.BlockSpec(memory_space=pltpu.VMEM)
        hbm = pl.BlockSpec(memory_space=pl.ANY)
        act = jax.ShapeDtypeStruct((samples, seq, width), jnp.bfloat16)
        x_part = jax.ShapeDtypeStruct((samples, seq // stages, width), jnp.bfloat16)
        bf = jnp.bfloat16
        x_out, k_new, v_new, _ = pl.pallas_call(
            functools.partial(stage_kernel, stages, UNITS, head_dim),
            out_shape=(x_part, act, act, act),
            in_specs=[hbm] + [vmem] * 7 + [hbm] * 4,
            out_specs=(hbm, hbm, hbm, hbm),
            scratch_shapes=[
                pltpu.VMEM((WEIGHT_SLOTS, width, width), bf),
                pltpu.VMEM((seq, width), bf), pltpu.VMEM((seq, width), bf),
                pltpu.VMEM((rows, width), bf),
                pltpu.VMEM((3, rows, width), bf),
                pltpu.VMEM((tiles_two, rows, width), bf),
                pltpu.VMEM((rows, width), jnp.float32),
                pltpu.VMEM((rows, width), bf),
                pltpu.SemaphoreType.DMA((WEIGHT_SLOTS,)),
                pltpu.SemaphoreType.DMA((2,)),
                pltpu.SemaphoreType.DMA,
                pltpu.SemaphoreType.DMA((2,)),
                pltpu.SemaphoreType.DMA,
                pltpu.SemaphoreType.DMA,
                pltpu.SemaphoreType.DMA((chunks,)),
                pltpu.SemaphoreType.DMA((samples,)),
            ],
            compiler_params=pltpu.CompilerParams(collective_id=0, has_side_effects=True, vmem_limit_bytes=67043328),
            name='stage_kernel',
        )(x_in.reshape(samples, seq, width), mod, b_one.astype(jnp.float32).reshape(tiles_one, 1, width), gains, cos_tab, sin_tab, ones_bd,
          b_two.astype(jnp.float32), w_one[0], w_two[0], k_prev.reshape(samples, seq, width), v_prev.reshape(samples, seq, width))
        x_out = x_out.reshape(samples, patches // stages, patch_tok, width)
        return x_out, k_new.reshape(k_prev.shape), v_new.reshape(v_prev.shape)

    return jax.shard_map(
        stage_program, mesh=mesh,
        in_specs=(P('dp'), P('dp'), P(), P('pp'), P('pp'), P('pp'), P('pp'), P('pp'), P('pp'), P('pp'), P('pp', 'dp'), P('pp', 'dp')),
        out_specs=(P('dp', 'pp'), P('pp', 'dp'), P('pp', 'dp')),
        check_vma=False)
```

```python
import functools
import math
import jax
import jax.numpy as jnp
from jax import lax
from jax.experimental import pallas as pl
from jax.experimental.pallas import tpu as pltpu
from jax.sharding import PartitionSpec as P

UNITS = 2
WEIGHT_SLOTS = 4
LANES = 128
SOFT_ROWS = 16


def rope_tables(pos_ids, head_dim):
    axis_zero = head_dim // 8
    axis_rest = (head_dim - axis_zero) // 2
    pieces = []
    for axis_idx, axis_dim in enumerate((axis_zero, axis_rest, head_dim - axis_zero - axis_rest)):
        axis_freqs = 1.0 / (10000.0 ** (jnp.arange(0, axis_dim, 2, dtype=jnp.float32) / axis_dim))
        pieces.append(pos_ids[..., axis_idx:axis_idx + 1].astype(jnp.float32) * axis_freqs)
    angles = jnp.concatenate(pieces, axis=-1)
    return jnp.cos(angles), jnp.sin(angles)


def tile_halves(width):
    second = max(width // (4 * LANES) // 2, 1) * 4 * LANES if width >= 8 * LANES else LANES
    return ((0, width - second), (width - second, second))


def stage_kernel(stages, units, head_dim,
                 x_in, mod, b_one, gains, cos_tab, sin_tab, ones_bd, b_two, w_one, w_two, k_prev, v_prev,
                 x_out, k_new, v_new,
                 w_buf, k_buf, v_buf, x_buf, qkv, joined, acc, o_buf, score0, score1, prob0, prob1,
                 w_sem, kv_sem, x_sem, kv_out_sem, send_sem, local_sem, recv_sem, out_sem, free_sem):
    stage = lax.axis_index('pp')
    samples, seq, width = x_in.shape
    rows = x_buf.shape[1]
    patch_tok = rows // units
    parts = seq // rows
    chunks = samples * parts
    slots = w_buf.shape[0]
    tiles_one = w_one.shape[1] // width
    tiles_two = w_two.shape[0] // width
    tiles = tiles_one + tiles_two
    last = stages - 1

    barrier = pltpu.get_barrier_semaphore()
    for hop in range(1, stages):
        pl.semaphore_signal(barrier, inc=1, device_id={'pp': lax.rem(stage + hop, stages)}, device_id_type=pl.DeviceIdType.MESH)
    pl.semaphore_wait(barrier, stages - 1)

    halves = tile_halves(width)

    def half_start(g, half):
        off, size = halves[half]
        t = lax.rem(lax.div(g, 2), tiles)
        slot = lax.rem(g, slots)
        dst = w_buf.at[slot, :, pl.ds(0, size)]

        @pl.when(t < tiles_one)
        def _():
            pltpu.make_async_copy(w_one.at[:, pl.ds(pl.multiple_of(t * width + off, LANES), size)], dst, w_sem.at[slot]).start()

        @pl.when(t >= tiles_one)
        def _():
            pltpu.make_async_copy(w_two.at[pl.ds(pl.multiple_of((t - tiles_one) * width, LANES), width), pl.ds(off, size)], dst, w_sem.at[slot]).start()

    def run_tile(tile, body):
        for half, (off, size) in enumerate(halves):
            g = 2 * tile + half
            slot = lax.rem(g, slots)
            weights = w_buf.at[slot, :, pl.ds(0, size)]
            pltpu.make_async_copy(w_two.at[pl.ds(0, width), pl.ds(off, size)], weights, w_sem.at[slot]).wait()
            body(weights, off, size)

            @pl.when(g + slots < 2 * chunks * tiles)
            def _():
                half_start(g + slots, (half + slots) % 2)

    for g0 in range(slots):
        half_start(g0, g0 % 2)

    def send_copy(c):
        return pltpu.make_async_remote_copy(
            src_ref=o_buf, dst_ref=x_buf.at[lax.rem(c, 2)],
            send_sem=send_sem, recv_sem=recv_sem.at[c],
            device_id={'pp': lax.rem(stage + 1, stages)}, device_id_type=pl.DeviceIdType.MESH)

    def out_copy(c):
        s, part = lax.div(c, parts), lax.rem(c, parts)
        return pltpu.make_async_remote_copy(
            src_ref=o_buf, dst_ref=x_out.at[s], send_sem=send_sem, recv_sem=out_sem.at[s],
            device_id={'pp': part}, device_id_type=pl.DeviceIdType.MESH)

    def local_copy(c):
        return pltpu.make_async_copy(o_buf, x_out.at[lax.div(c, parts)], local_sem)

    def out_start(c):
        part = lax.rem(c, parts)

        @pl.when(stage < last)
        def _():
            @pl.when(c >= 2)
            def _():
                pl.semaphore_wait(free_sem, 1)

            send_copy(c).start()

        @pl.when((stage == last) & (part < last))
        def _():
            out_copy(c).start()

        @pl.when((stage == last) & (part == last))
        def _():
            local_copy(c).start()

    def out_wait(c):
        part = lax.rem(c, parts)

        @pl.when(stage < last)
        def _():
            send_copy(c).wait_send()

        @pl.when((stage == last) & (part < last))
        def _():
            out_copy(c).wait_send()

        @pl.when((stage == last) & (part == last))
        def _():
            local_copy(c).wait()

    def in_copy(c):
        s, part = lax.div(c, parts), lax.rem(c, parts)
        slot = lax.rem(c, 2)
        return pltpu.make_async_copy(x_in.at[s, pl.ds(pl.multiple_of(part * rows, LANES), rows), :], x_buf.at[slot], x_sem.at[slot])

    @pl.when(stage == 0)
    def _():
        in_copy(0).start()

    lane = lax.broadcasted_iota(jnp.int32, (patch_tok, LANES), 1)
    low_half = (lane < head_dim)
    low_bf = low_half.astype(jnp.float32).astype(jnp.bfloat16)
    high_bf = (1.0 - low_half.astype(jnp.float32)).astype(jnp.bfloat16)

    def chunk_body(c, carry):
        s, part = lax.div(c, parts), lax.rem(c, parts)
        row0 = pl.multiple_of(part * rows, LANES)
        base = c * tiles
        span = pl.ds(row0, rows)

        def prev_copies():
            return (pltpu.make_async_copy(k_prev.at[s], k_buf, kv_sem.at[0]),
                    pltpu.make_async_copy(v_prev.at[s], v_buf, kv_sem.at[1]))

        @pl.when(part == 0)
        def _():
            for cp in prev_copies():
                cp.start()

        @pl.when(stage == 0)
        def _():
            in_copy(c).wait()

            @pl.when(c + 1 < chunks)
            def _():
                in_copy(c + 1).start()

        @pl.when(stage > 0)
        def _():
            send_copy(c).wait_recv()

        x_now = x_buf.at[lax.rem(c, 2)]
        norm_rows = 16

        def norm_step(r, carry):
            at = pl.ds(pl.multiple_of(r * norm_rows, norm_rows), norm_rows)
            act = x_now[at, :].astype(jnp.float32)
            centered = act - jnp.mean(act, axis=-1, keepdims=True)
            normed = centered * lax.rsqrt(jnp.mean(centered * centered, axis=-1, keepdims=True) + 1e-6)
            joined[0, at, :] = (normed * (1.0 + mod[s, 1:2, :]) + mod[s, 0:1, :]).astype(jnp.bfloat16)
            return carry

        lax.fori_loop(0, rows // norm_rows, norm_step, 0, unroll=4)

        def proj(weights, j, off, size):
            out = jnp.dot(joined[0], weights[...], preferred_element_type=jnp.float32)
            return (out + b_one[j, :, pl.ds(off, size)]).astype(jnp.bfloat16)

        def head_tile(j, carry):
            even = (lax.broadcasted_iota(jnp.int32, (rows, LANES), 1) & 1) == 0

            def rotate(raw, off):
                cos_v = cos_tab[span, :]
                sin_v = sin_tab[span, :]
                size = raw.shape[1]
                for lo in range(0, size, 2 * LANES):
                    wide = min(2 * LANES, size - lo)
                    sub = raw[:, lo:lo + wide].astype(jnp.float32)
                    sq = sub * sub
                    ones = ones_bd[:wide, :wide]
                    sq0 = sq.astype(jnp.bfloat16)
                    sq1 = (sq - sq0.astype(jnp.float32)).astype(jnp.bfloat16)
                    total = jnp.dot(sq0, ones, preferred_element_type=jnp.float32)
                    total += jnp.dot(sq1, ones, preferred_element_type=jnp.float32)
                    inv = lax.rsqrt(total * (1.0 / head_dim) + 1e-6)
                    for l2 in range(0, wide, LANES):
                        one = sub[:, l2:l2 + LANES] * inv[:, l2:l2 + LANES] * gains[j]
                        swapped = jnp.where(even, pltpu.roll(one, LANES - 1, 1), pltpu.roll(one, 1, 1))
                        rot = one * cos_v + swapped * sin_v
                        qkv[j, :, off + lo + l2:off + lo + l2 + LANES] = rot.astype(jnp.bfloat16)

            def body(weights, off, size):
                waiting = None
                for lo in range(0, size, 4 * LANES):
                    wide = min(4 * LANES, size - lo)
                    fresh = (proj(weights.at[:, pl.ds(lo, wide)], j, off + lo, wide), off + lo)
                    if waiting is not None:
                        rotate(*waiting)
                    waiting = fresh
                rotate(*waiting)

            run_tile(base + j, body)
            return carry

        lax.fori_loop(0, 2, head_tile, 0)

        def value_body(weights, off, size):
            qkv[2, :, pl.ds(off, size)] = proj(weights, 2, off, size)

        run_tile(base + 2, value_body)

        def fresh_copies():
            return (pltpu.make_async_copy(qkv.at[1], k_new.at[s, span, :], kv_out_sem.at[0]),
                    pltpu.make_async_copy(qkv.at[2], v_new.at[s, span, :], kv_out_sem.at[1]))

        for cp in fresh_copies():
            cp.start()

        def mlp_tile(j, carry):
            def body(weights, off, size):
                pre = proj(weights, j, off, size).astype(jnp.float32)
                joined[j - 2, :, pl.ds(off, size)] = jax.nn.gelu(pre, approximate=True).astype(jnp.bfloat16)

            run_tile(base + j, body)
            return carry

        lax.fori_loop(3, tiles_one, mlp_tile, 0)

        @pl.when(part == 0)
        def _():
            for cp in prev_copies():
                cp.wait()

        def unit_step(u, carry):
            q_rows = pl.ds(pl.multiple_of(u * patch_tok, LANES), patch_tok)
            key_rows = pl.ds(pl.multiple_of(row0 + u * patch_tok, LANES), patch_tok)
            k_buf[key_rows, :] = qkv[1, q_rows, :]
            v_buf[key_rows, :] = qkv[2, q_rows, :]

            pairs = width // LANES
            quads = -(-pairs // 2)
            two_rows = 2 * patch_tok

            def first_pair(quad):
                return min(2 * quad, pairs - 2)

            def score(quad, which, dst):
                cols = pl.ds((first_pair(quad) + which) * LANES, LANES)
                q2 = qkv[0, q_rows, cols]
                both = jnp.concatenate([q2 * low_bf, q2 * high_bf], axis=0)
                dst[...] = lax.dot_general(both, k_buf[:, cols], (((1,), (1,)), ((), ())), preferred_element_type=jnp.float32)

            def soften(which, src, dst):
                for r in range(0, two_rows, SOFT_ROWS):
                    sc = src[r:r + SOFT_ROWS, :]
                    ex = jnp.exp(sc - jnp.max(sc, axis=-1, keepdims=True))
                    at = which * two_rows + r
                    dst[at:at + SOFT_ROWS, :] = (ex * (1.0 / jnp.sum(ex, axis=-1, keepdims=True))).astype(jnp.bfloat16)

            def mix(quad, src):
                cols = pl.ds(first_pair(quad) * LANES, 2 * LANES)
                mixed = jnp.dot(src[...], v_buf[:, cols], preferred_element_type=jnp.float32)
                t = patch_tok
                out = jnp.concatenate([jnp.where(low_half, mixed[:t, :LANES], mixed[t:2 * t, :LANES]),
                                       jnp.where(low_half, mixed[2 * t:3 * t, LANES:], mixed[3 * t:, LANES:])], axis=1)
                joined[0, q_rows, cols] = out.astype(jnp.bfloat16)

            def quad_step(quad, before, now):
                if before is not None:
                    mix(quad - 1, before)
                for which, buf in enumerate((score0, score1)):
                    soften(which, buf, now)
                    if quad + 1 < quads:
                        score(quad + 1, which, buf)

            score(0, 0, score0)
            score(0, 1, score1)
            quad_step(0, None, prob0)

            probs = (prob0, prob1)
            for quad in range(1, quads):
                quad_step(quad, probs[1 - quad % 2], probs[quad % 2])
            mix(quads - 1, probs[(quads - 1) % 2])
            return carry

        lax.fori_loop(0, units, unit_step, 0)

        def two_tile(j, carry):
            def body(weights, off, size):
                cols = pl.ds(off, size)
                acc[:, cols] = acc[:, cols] + jnp.dot(joined[j], weights[...], preferred_element_type=jnp.float32)

            run_tile(base + tiles_one + j, body)
            return carry

        acc[...] = jnp.zeros_like(acc)
        lax.fori_loop(0, tiles_two, two_tile, 0)

        for cp in fresh_copies():
            cp.wait()

        @pl.when(c > 0)
        def _():
            out_wait(c - 1)

        def res_step(r, carry):
            at = pl.ds(pl.multiple_of(r * norm_rows, norm_rows), norm_rows)
            block_out = acc[at, :] + b_two[...]
            o_buf[at, :] = (x_now[at, :].astype(jnp.float32) + mod[s, 2:3, :] * block_out).astype(jnp.bfloat16)
            return carry

        lax.fori_loop(0, rows // norm_rows, res_step, 0, unroll=2)
        @pl.when((stage > 0) & (c + 2 < chunks))
        def _():
            pl.semaphore_signal(free_sem, inc=1, device_id={'pp': lax.rem(stage + stages - 1, stages)}, device_id_type=pl.DeviceIdType.MESH)

        out_start(c)
        return carry

    lax.fori_loop(0, chunks, chunk_body, 0)
    out_wait(chunks - 1)

    @pl.when(stage < last)
    def _():
        for s in range(samples):
            out_copy(s * parts).wait_recv()


def solution(mesh):
    stages = mesh.shape['pp']

    def stage_program(x_in, cond_vec, pos_ids, w_mod, b_mod, w_one, b_one, qk_scale, w_two, b_two, k_prev, v_prev):
        samples, patches, patch_tok, width = x_in.shape
        head_dim = qk_scale.shape[-1]
        seq = patches * patch_tok
        rows = UNITS * patch_tok
        chunks = samples * seq // rows
        tiles_one = w_one.shape[2] // width
        tiles_two = w_two.shape[1] // width
        cond_act = jax.nn.silu(cond_vec.astype(jnp.float32)).astype(jnp.bfloat16)
        mod = jnp.dot(cond_act, w_mod[0], preferred_element_type=jnp.float32) + b_mod.astype(jnp.float32)
        mod = mod.reshape(samples, 3, width)
        cos_tab, sin_tab = rope_tables(pos_ids.reshape(seq, 3), head_dim)
        heads_in_lane = LANES // head_dim
        cos_tab = jnp.tile(jnp.repeat(cos_tab, 2, axis=-1), (1, heads_in_lane))
        sin_tab = jnp.stack([-sin_tab, sin_tab], axis=-1).reshape(seq, head_dim)
        sin_tab = jnp.tile(sin_tab, (1, heads_in_lane))
        scale = jnp.array([1.0 / math.sqrt(head_dim), 1.0], jnp.float32)
        gains = jnp.tile(qk_scale[0].astype(jnp.float32) * scale[:, None], (1, heads_in_lane)).reshape(2, 1, LANES)
        group = jnp.arange(2 * LANES) // head_dim
        ones_bd = (group[:, None] == group[None, :]).astype(jnp.bfloat16)
        vmem = pl.BlockSpec(memory_space=pltpu.VMEM)
        hbm = pl.BlockSpec(memory_space=pl.ANY)
        act = jax.ShapeDtypeStruct((samples, seq, width), jnp.bfloat16)
        x_part = jax.ShapeDtypeStruct((samples, seq // stages, width), jnp.bfloat16)
        bf = jnp.bfloat16
        x_out, k_new, v_new = pl.pallas_call(
            functools.partial(stage_kernel, stages, UNITS, head_dim),
            out_shape=(x_part, act, act),
            in_specs=[hbm] + [vmem] * 7 + [hbm] * 4,
            out_specs=(hbm, hbm, hbm),
            scratch_shapes=[
                pltpu.VMEM((WEIGHT_SLOTS, width, tile_halves(width)[0][1]), bf),
                pltpu.VMEM((seq, width), bf), pltpu.VMEM((seq, width), bf),
                pltpu.VMEM((2, rows, width), bf),
                pltpu.VMEM((3, rows, width), bf),
                pltpu.VMEM((tiles_two, rows, width), bf),
                pltpu.VMEM((rows, width), jnp.float32),
                pltpu.VMEM((rows, width), bf),
                pltpu.VMEM((2 * patch_tok, seq), jnp.float32), pltpu.VMEM((2 * patch_tok, seq), jnp.float32),
                pltpu.VMEM((4 * patch_tok, seq), bf), pltpu.VMEM((4 * patch_tok, seq), bf),
                pltpu.SemaphoreType.DMA((WEIGHT_SLOTS,)),
                pltpu.SemaphoreType.DMA((2,)),
                pltpu.SemaphoreType.DMA((2,)),
                pltpu.SemaphoreType.DMA((2,)),
                pltpu.SemaphoreType.DMA,
                pltpu.SemaphoreType.DMA,
                pltpu.SemaphoreType.DMA((chunks,)),
                pltpu.SemaphoreType.DMA((samples,)),
                pltpu.SemaphoreType.REGULAR,
            ],
            compiler_params=pltpu.CompilerParams(collective_id=0, has_side_effects=True, vmem_limit_bytes=67043328),
            name='stage_kernel',
        )(x_in.reshape(samples, seq, width), mod, b_one.astype(jnp.float32).reshape(tiles_one, 1, width), gains, cos_tab, sin_tab, ones_bd,
          b_two.astype(jnp.float32), w_one[0], w_two[0], k_prev.reshape(samples, seq, width), v_prev.reshape(samples, seq, width))
        x_out = x_out.reshape(samples, patches // stages, patch_tok, width)
        return x_out, k_new.reshape(k_prev.shape), v_new.reshape(v_prev.shape)

    return jax.shard_map(
        stage_program, mesh=mesh,
        in_specs=(P('dp'), P('dp'), P(), P('pp'), P('pp'), P('pp'), P('pp'), P('pp'), P('pp'), P('pp'), P('pp', 'dp'), P('pp', 'dp')),
        out_specs=(P('dp', 'pp'), P('pp', 'dp'), P('pp', 'dp')),
        check_vma=False)
```

```python
import functools
import math
import jax
import jax.numpy as jnp
import numpy as np
from jax import lax
from jax.experimental import pallas as pl
from jax.experimental.pallas import tpu as pltpu
from jax.sharding import PartitionSpec as P

UNITS = 2
WEIGHT_SLOTS = 4
LANES = 128
SOFT_ROWS = 16


def rope_tables(pos_ids, head_dim, lanes):
    axis_zero = head_dim // 8
    axis_rest = (head_dim - axis_zero) // 2
    freqs, axes = [], []
    for axis_idx, axis_dim in enumerate((axis_zero, axis_rest, head_dim - axis_zero - axis_rest)):
        freqs.append(1.0 / (10000.0 ** (jnp.arange(0, axis_dim, 2, dtype=jnp.float32) / axis_dim)))
        axes += [axis_idx] * axis_dim
    lane_freq = jnp.tile(jnp.repeat(jnp.concatenate(freqs), 2), lanes // head_dim)
    axis = jnp.array(axes * (lanes // head_dim), jnp.int32)
    pos = pos_ids.astype(jnp.float32)
    lane_pos = jnp.where(axis == 0, pos[:, 0:1], jnp.where(axis == 1, pos[:, 1:2], pos[:, 2:3]))
    angles = lane_pos * lane_freq
    sign = jnp.where(jnp.arange(lanes) % 2 == 0, -1.0, 1.0)
    return jnp.cos(angles), jnp.sin(angles) * sign


def tile_halves(width):
    second = max(width // (4 * LANES) // 2, 1) * 4 * LANES if width >= 8 * LANES else LANES
    return ((0, width - second), (width - second, second))


def stage_kernel(stages, units, head_dim,
                 x_in, mod, b_one, gains, cos_tab, sin_tab, ones_bd, b_two, w_one, w_two, k_prev, v_prev,
                 x_out, k_new, v_new,
                 w_buf, k_buf, v_buf, x_buf, qkv, joined, acc, o_buf, score0, score1, prob0, prob1,
                 w_sem, kv_sem, x_sem, kv_out_sem, send_sem, local_sem, recv_sem, out_sem, free_sem):
    stage = lax.axis_index('pp')
    samples, seq, width = x_in.shape
    rows = x_buf.shape[1]
    patch_tok = rows // units
    parts = seq // rows
    chunks = samples * parts
    slots = w_buf.shape[0]
    tiles_one = w_one.shape[1] // width
    tiles_two = w_two.shape[0] // width
    tiles = tiles_one + tiles_two
    last = stages - 1

    barrier = pltpu.get_barrier_semaphore()
    for hop in range(1, stages):
        pl.semaphore_signal(barrier, inc=1, device_id={'pp': lax.rem(stage + hop, stages)}, device_id_type=pl.DeviceIdType.MESH)
    pl.semaphore_wait(barrier, stages - 1)

    halves = tile_halves(width)

    def half_start(g, half):
        off, size = halves[half]
        t = lax.rem(lax.div(g, 2), tiles)
        slot = lax.rem(g, slots)
        dst = w_buf.at[slot, :, pl.ds(0, size)]

        @pl.when(t < tiles_one)
        def _():
            pltpu.make_async_copy(w_one.at[:, pl.ds(pl.multiple_of(t * width + off, LANES), size)], dst, w_sem.at[slot]).start()

        @pl.when(t >= tiles_one)
        def _():
            pltpu.make_async_copy(w_two.at[pl.ds(pl.multiple_of((t - tiles_one) * width, LANES), width), pl.ds(off, size)], dst, w_sem.at[slot]).start()

    def run_tile(tile, body):
        for half, (off, size) in enumerate(halves):
            g = 2 * tile + half
            slot = lax.rem(g, slots)
            weights = w_buf.at[slot, :, pl.ds(0, size)]
            pltpu.make_async_copy(w_two.at[pl.ds(0, width), pl.ds(off, size)], weights, w_sem.at[slot]).wait()
            body(weights, off, size)

            @pl.when(g + slots < 2 * chunks * tiles)
            def _():
                half_start(g + slots, (half + slots) % 2)

    for g0 in range(slots):
        half_start(g0, g0 % 2)

    def send_copy(c):
        return pltpu.make_async_remote_copy(
            src_ref=o_buf, dst_ref=x_buf.at[lax.rem(c, 2)],
            send_sem=send_sem, recv_sem=recv_sem.at[c],
            device_id={'pp': lax.rem(stage + 1, stages)}, device_id_type=pl.DeviceIdType.MESH)

    def out_copy(c):
        s, part = lax.div(c, parts), lax.rem(c, parts)
        return pltpu.make_async_remote_copy(
            src_ref=o_buf, dst_ref=x_out.at[s], send_sem=send_sem, recv_sem=out_sem.at[s],
            device_id={'pp': part}, device_id_type=pl.DeviceIdType.MESH)

    def local_copy(c):
        return pltpu.make_async_copy(o_buf, x_out.at[lax.div(c, parts)], local_sem)

    def out_start(c):
        part = lax.rem(c, parts)

        @pl.when(stage < last)
        def _():
            @pl.when(c >= 2)
            def _():
                pl.semaphore_wait(free_sem, 1)

            send_copy(c).start()

        @pl.when((stage == last) & (part < last))
        def _():
            out_copy(c).start()

        @pl.when((stage == last) & (part == last))
        def _():
            local_copy(c).start()

    def out_wait(c):
        part = lax.rem(c, parts)

        @pl.when(stage < last)
        def _():
            send_copy(c).wait_send()

        @pl.when((stage == last) & (part < last))
        def _():
            out_copy(c).wait_send()

        @pl.when((stage == last) & (part == last))
        def _():
            local_copy(c).wait()

    def in_copy(c):
        s, part = lax.div(c, parts), lax.rem(c, parts)
        slot = lax.rem(c, 2)
        return pltpu.make_async_copy(x_in.at[s, pl.ds(pl.multiple_of(part * rows, LANES), rows), :], x_buf.at[slot], x_sem.at[slot])

    @pl.when(stage == 0)
    def _():
        in_copy(0).start()

    lane = lax.broadcasted_iota(jnp.int32, (patch_tok, LANES), 1)
    low_half = (lane < head_dim)
    low_bf = low_half.astype(jnp.float32).astype(jnp.bfloat16)
    high_bf = (1.0 - low_half.astype(jnp.float32)).astype(jnp.bfloat16)

    def chunk_body(c, carry):
        s, part = lax.div(c, parts), lax.rem(c, parts)
        row0 = pl.multiple_of(part * rows, LANES)
        base = c * tiles
        span = pl.ds(row0, rows)

        def prev_copies():
            return (pltpu.make_async_copy(k_prev.at[s], k_buf, kv_sem.at[0]),
                    pltpu.make_async_copy(v_prev.at[s], v_buf, kv_sem.at[1]))

        @pl.when(stage == 0)
        def _():
            in_copy(c).wait()

            @pl.when(c + 1 < chunks)
            def _():
                in_copy(c + 1).start()

        @pl.when(stage > 0)
        def _():
            send_copy(c).wait_recv()

        x_now = x_buf.at[lax.rem(c, 2)]
        norm_rows = 16

        def norm_step(r, carry):
            at = pl.ds(pl.multiple_of(r * norm_rows, norm_rows), norm_rows)
            act = x_now[at, :].astype(jnp.float32)
            centered = act - jnp.mean(act, axis=-1, keepdims=True)
            normed = centered * lax.rsqrt(jnp.mean(centered * centered, axis=-1, keepdims=True) + 1e-6)
            joined[0, at, :] = (normed * (1.0 + mod[s, 1:2, :]) + mod[s, 0:1, :]).astype(jnp.bfloat16)
            return carry

        lax.fori_loop(0, rows // norm_rows, norm_step, 0, unroll=4)

        def proj(weights, j, off, size):
            out = jnp.dot(joined[0], weights[...], preferred_element_type=jnp.float32)
            return (out + b_one[j, :, pl.ds(off, size)].astype(jnp.float32)).astype(jnp.bfloat16)

        def raw_tile(j, carry):
            def body(weights, off, size):
                qkv[j, :, pl.ds(off, size)] = proj(weights, j, off, size)

            run_tile(base + j, body)
            return carry

        def fresh_copies():
            return (pltpu.make_async_copy(qkv.at[1], k_new.at[s, span, :], kv_out_sem.at[0]),
                    pltpu.make_async_copy(qkv.at[2], v_new.at[s, span, :], kv_out_sem.at[1]))

        even = (lax.broadcasted_iota(jnp.int32, (rows, LANES), 1) & 1) == 0

        def head_norm(j):
            def rotate(off, size):
                cos_v = cos_tab[span, :]
                sin_v = sin_tab[span, :]
                for lo in range(0, size, 2 * LANES):
                    wide = min(2 * LANES, size - lo)
                    sub = qkv[j, :, off + lo:off + lo + wide].astype(jnp.float32)
                    sq = sub * sub
                    ones = ones_bd[:wide, :wide]
                    sq0 = sq.astype(jnp.bfloat16)
                    sq1 = (sq - sq0.astype(jnp.float32)).astype(jnp.bfloat16)
                    total = jnp.dot(sq0, ones, preferred_element_type=jnp.float32)
                    total += jnp.dot(sq1, ones, preferred_element_type=jnp.float32)
                    inv = lax.rsqrt(total * (1.0 / head_dim) + 1e-6)
                    for l2 in range(0, wide, LANES):
                        one = sub[:, l2:l2 + LANES] * inv[:, l2:l2 + LANES] * gains[j]
                        swapped = jnp.where(even, pltpu.roll(one, LANES - 1, 1), pltpu.roll(one, 1, 1))
                        rot = one * cos_v + swapped * sin_v
                        qkv[j, :, off + lo + l2:off + lo + l2 + LANES] = rot.astype(jnp.bfloat16)

            return rotate

        def mlp_block(weights, j, lo, off, wide):
            pre = proj(weights.at[:, pl.ds(lo, wide)], j, off + lo, wide).astype(jnp.float32)
            joined[j - 2, :, off + lo:off + lo + wide] = jax.nn.gelu(pre, approximate=True).astype(jnp.bfloat16)

        def mlp_head_tile(j, carry):
            rotate = head_norm(j - 3)

            def body(weights, off, size):
                rotate(off, size)
                mlp_block(weights, j, 0, off, size)

            run_tile(base + j, body)
            return carry

        def mlp_tile(j, carry):
            run_tile(base + j, lambda weights, off, size: mlp_block(weights, j, 0, off, size))
            return carry

        lax.fori_loop(0, 3, raw_tile, 0)

        @pl.when(part == 0)
        def _():
            for cp in prev_copies():
                cp.start()

        lax.fori_loop(3, 5, mlp_head_tile, 0)

        for cp in fresh_copies():
            cp.start()

        lax.fori_loop(5, tiles_one, mlp_tile, 0)

        @pl.when(part == 0)
        def _():
            for cp in prev_copies():
                cp.wait()

        def unit_step(u, carry):
            q_rows = pl.ds(pl.multiple_of(u * patch_tok, LANES), patch_tok)
            key_rows = pl.ds(pl.multiple_of(row0 + u * patch_tok, LANES), patch_tok)
            k_buf[key_rows, :] = qkv[1, q_rows, :]
            v_buf[key_rows, :] = qkv[2, q_rows, :]

            pairs = width // LANES
            quads = -(-pairs // 2)
            two_rows = 2 * patch_tok

            def filled(quad):
                return min(2, pairs - 2 * quad)

            def score(quad, which, dst):
                cols = pl.ds((2 * quad + which) * LANES, LANES)
                q2 = qkv[0, q_rows, cols]
                both = jnp.concatenate([q2 * low_bf, q2 * high_bf], axis=0)
                dst[...] = lax.dot_general(both, k_buf[:, cols], (((1,), (1,)), ((), ())), preferred_element_type=jnp.float32)

            def soften(which, src, dst):
                for r in range(0, two_rows, SOFT_ROWS):
                    sc = src[r:r + SOFT_ROWS, :]
                    ex = jnp.exp(sc - jnp.max(sc, axis=-1, keepdims=True))
                    at = which * two_rows + r
                    dst[at:at + SOFT_ROWS, :] = (ex * (1.0 / jnp.sum(ex, axis=-1, keepdims=True))).astype(jnp.bfloat16)

            def mix(quad, src):
                count = filled(quad)
                cols = pl.ds(2 * quad * LANES, count * LANES)
                mixed = jnp.dot(src[:count * two_rows, :], v_buf[:, cols], preferred_element_type=jnp.float32)
                for which in range(count):
                    lanes = slice(which * LANES, (which + 1) * LANES)
                    top = which * two_rows
                    out = jnp.where(low_half, mixed[top:top + patch_tok, lanes], mixed[top + patch_tok:top + two_rows, lanes])
                    joined[0, q_rows, pl.ds((2 * quad + which) * LANES, LANES)] = out.astype(jnp.bfloat16)

            buffers = (score0, score1)
            probs = (prob0, prob1)
            for which in range(filled(0)):
                score(0, which, buffers[which])
            for quad in range(quads):
                if quad:
                    mix(quad - 1, probs[(quad - 1) % 2])
                for which in range(2):
                    if which < filled(quad):
                        soften(which, buffers[which], probs[quad % 2])
                    if quad + 1 < quads and which < filled(quad + 1):
                        score(quad + 1, which, buffers[which])
            mix(quads - 1, probs[(quads - 1) % 2])
            return carry

        lax.fori_loop(0, units, unit_step, 0)

        def two_tile(j, carry):
            def body(weights, off, size):
                cols = pl.ds(off, size)
                acc[:, cols] = acc[:, cols] + jnp.dot(joined[j], weights[...], preferred_element_type=jnp.float32)

            run_tile(base + tiles_one + j, body)
            return carry

        acc[...] = jnp.zeros_like(acc)
        lax.fori_loop(0, tiles_two, two_tile, 0)

        for cp in fresh_copies():
            cp.wait()

        @pl.when(c > 0)
        def _():
            out_wait(c - 1)

        def res_step(r, carry):
            at = pl.ds(pl.multiple_of(r * norm_rows, norm_rows), norm_rows)
            block_out = acc[at, :] + b_two[...].astype(jnp.float32)
            o_buf[at, :] = (x_now[at, :].astype(jnp.float32) + mod[s, 2:3, :] * block_out).astype(jnp.bfloat16)
            return carry

        lax.fori_loop(0, rows // norm_rows, res_step, 0, unroll=2)
        @pl.when((stage > 0) & (c + 2 < chunks))
        def _():
            pl.semaphore_signal(free_sem, inc=1, device_id={'pp': lax.rem(stage + stages - 1, stages)}, device_id_type=pl.DeviceIdType.MESH)

        out_start(c)
        return carry

    lax.fori_loop(0, chunks, chunk_body, 0)
    out_wait(chunks - 1)

    @pl.when(stage < last)
    def _():
        for s in range(samples):
            out_copy(s * parts).wait_recv()


def solution(mesh):
    stages = mesh.shape['pp']

    def stage_program(x_in, cond_vec, pos_ids, w_mod, b_mod, w_one, b_one, qk_scale, w_two, b_two, k_prev, v_prev):
        samples, patches, patch_tok, width = x_in.shape
        head_dim = qk_scale.shape[-1]
        seq = patches * patch_tok
        rows = UNITS * patch_tok
        chunks = samples * seq // rows
        tiles_one = w_one.shape[2] // width
        tiles_two = w_two.shape[1] // width
        cond_act = jax.nn.silu(cond_vec.astype(jnp.float32)).astype(jnp.bfloat16)
        mod = jnp.dot(cond_act, w_mod[0], preferred_element_type=jnp.float32) + b_mod.astype(jnp.float32)
        mod = mod.reshape(samples, 3, width)
        cos_tab, sin_tab = rope_tables(pos_ids.reshape(seq, 3), head_dim, LANES)
        heads_in_lane = LANES // head_dim
        scale = jnp.array([1.0 / math.sqrt(head_dim), 1.0], jnp.float32)
        gains = jnp.tile(qk_scale[0].astype(jnp.float32) * scale[:, None], (1, heads_in_lane)).reshape(2, 1, LANES)
        group = np.arange(2 * LANES) // head_dim
        ones_bd = jnp.asarray(group[:, None] == group[None, :], jnp.bfloat16)
        vmem = pl.BlockSpec(memory_space=pltpu.VMEM)
        hbm = pl.BlockSpec(memory_space=pl.ANY)
        act = jax.ShapeDtypeStruct((samples, seq, width), jnp.bfloat16)
        x_part = jax.ShapeDtypeStruct((samples, seq // stages, width), jnp.bfloat16)
        bf = jnp.bfloat16
        x_out, k_new, v_new = pl.pallas_call(
            functools.partial(stage_kernel, stages, UNITS, head_dim),
            out_shape=(x_part, act, act),
            in_specs=[hbm] + [vmem] * 7 + [hbm] * 4,
            out_specs=(hbm, hbm, hbm),
            scratch_shapes=[
                pltpu.VMEM((WEIGHT_SLOTS, width, tile_halves(width)[0][1]), bf),
                pltpu.VMEM((seq, width), bf), pltpu.VMEM((seq, width), bf),
                pltpu.VMEM((2, rows, width), bf),
                pltpu.VMEM((3, rows, width), bf),
                pltpu.VMEM((tiles_two, rows, width), bf),
                pltpu.VMEM((rows, width), jnp.float32),
                pltpu.VMEM((rows, width), bf),
                pltpu.VMEM((2 * patch_tok, seq), jnp.float32), pltpu.VMEM((2 * patch_tok, seq), jnp.float32),
                pltpu.VMEM((4 * patch_tok, seq), bf), pltpu.VMEM((4 * patch_tok, seq), bf),
                pltpu.SemaphoreType.DMA((WEIGHT_SLOTS,)),
                pltpu.SemaphoreType.DMA((2,)),
                pltpu.SemaphoreType.DMA((2,)),
                pltpu.SemaphoreType.DMA((2,)),
                pltpu.SemaphoreType.DMA,
                pltpu.SemaphoreType.DMA,
                pltpu.SemaphoreType.DMA((chunks,)),
                pltpu.SemaphoreType.DMA((samples,)),
                pltpu.SemaphoreType.REGULAR,
            ],
            compiler_params=pltpu.CompilerParams(collective_id=0, has_side_effects=True, vmem_limit_bytes=67043328),
            name='stage_kernel',
        )(x_in.reshape(samples, seq, width), mod, b_one.reshape(tiles_one, 1, width), gains, cos_tab, sin_tab, ones_bd,
          b_two, w_one[0], w_two[0], k_prev.reshape(samples, seq, width), v_prev.reshape(samples, seq, width))
        x_out = x_out.reshape(samples, patches // stages, patch_tok, width)
        return x_out, k_new.reshape(k_prev.shape), v_new.reshape(v_prev.shape)

    return jax.shard_map(
        stage_program, mesh=mesh,
        in_specs=(P('dp'), P('dp'), P(), P('pp'), P('pp'), P('pp'), P('pp'), P('pp'), P('pp'), P('pp'), P('pp', 'dp'), P('pp', 'dp')),
        out_specs=(P('dp', 'pp'), P('pp', 'dp'), P('pp', 'dp')),
        check_vma=False)
```
